128 devices in a mesh: gx: 4 (over x), gy: 8 (over z, y_lo), gz: 4 (over y_hi, core).
Axes of the slice: x: 4, y: 4 (y_hi: 2, y_lo: 2; y = y_hi * 2 + y_lo), z: 4, core: 2. Of those that a mesh axis runs over, the one named last changes fastest.
Arguments:
- tokens: bfloat16 [4096, 6144], P('gy', ('gz', 'gx')), may hold values from -6 to 6
- weight: bfloat16 [6144, 24576], P('gz', ('gx', 'gy')), may hold values from -0.15625 to 0.15625
- bias: float32 [24576], P(('gx', 'gz')), may hold values from -4 to 4
Outputs:
- hidden: bfloat16 [4096, 24576], P('gy', ('gx', 'gz'))
The draws below stay inside these ranges and needn't reach their ends.
All inputs are finite; a program needn't handle non-finite values.
Results may differ from the reference program's by a relative error of at most 0.001.
Values may be sent and summed in bfloat16 or wider, within the bound.
No kernel may reach another device: no remote copies, remote signals or barrier semaphores. Data moves between devices by JAX's collectives and lax.ppermute only.
A program may use at most 128 MiB of HBM per device.

```python
import jax
import jax.numpy as jnp

D = 6144
FF = 24576
TOKENS = 4096


def spiked(values, rng, source, target, shards_of, factor):
    owner, partner = [(jnp.arange(values.shape[axis_at]) // (values.shape[axis_at] // shards_of)).reshape([-1 if axis == axis_at else 1 for axis in range(values.ndim)]) for axis_at in (source, target)]
    chosen = jax.random.permutation(rng, shards_of)[partner]
    strong = (owner == chosen) | (owner == (partner + shards_of // 2) % shards_of)
    return jnp.where(strong, factor * values, values)


def level_of(key, dims, split, least, high):
    level = 1.0
    for position, shards_of in split:
        heights = jax.random.uniform(jax.random.fold_in(jax.random.fold_in(key, 6), position), (shards_of,), jnp.float32, least / len(split), high / len(split))
        level = level * jnp.repeat(jnp.exp(heights), dims[position] // shards_of).reshape((-1,) + (1,) * (len(dims) - 1 - position))
    return level


def scatter_about(key, extent, width, limit, shards=(), held_as=jnp.bfloat16):
    drawn = width * jax.random.normal(key, extent, jnp.float32)
    if shards:
        drawn = drawn * level_of(key, extent, shards, -0.22, 0.18)
    return jnp.clip(drawn, -limit, limit).astype(held_as)


def heavy_noise(stream_key, shape, spread, limit, cuts, heavy, kind=jnp.bfloat16):
    array = spread * jax.random.normal(stream_key, shape, jnp.float32)
    if cuts:
        array = array * level_of(stream_key, shape, cuts, -0.22, 0.18)
    return jnp.clip(spiked(array, jax.random.fold_in(stream_key, 3), *heavy), -limit, limit).astype(kind)


def setup_inputs(seed: int = 0) -> dict:
    key_list = jax.random.split(jax.random.key(seed), 4)
    return {
        "tokens": scatter_about(key_list[0], (TOKENS, D), 1.0, 6.0, ((0, 8), (1, 16))),
        "weight": heavy_noise(key_list[1], (D, FF), D ** -0.5, 0.15625, ((0, 4), (1, 32)), (0, 1, 32, 2.75)),
        "bias": scatter_about(key_list[2], (FF,), 1.0, 4.0, ((0, 16),), jnp.float32),
    }


def reference(tokens, weight, bias):
    pre = jnp.dot(tokens, weight, preferred_element_type=jnp.float32) + bias.astype(jnp.float32)
    return jax.nn.gelu(pre, approximate=False).astype(jnp.bfloat16)
```

```python
import jax
import jax.numpy as jnp
from jax import lax
from jax.experimental import pallas as pl
from jax.experimental.pallas import tpu as pltpu
from jax.sharding import Mesh
from jax.sharding import PartitionSpec as P


HALVES = ((0, 256), (256, 128))
VMEM = pl.BlockSpec(memory_space=pltpu.VMEM)
SMEM = pl.BlockSpec(memory_space=pltpu.SMEM)
HBM = pl.BlockSpec(memory_space=pl.ANY)
RING4 = {s: [(i, (i + s) % 4) for i in range(4)] for s in (1, 2, 3)}
SWAP = [(0, 1), (1, 0)]


def up(v, axis):
    return lax.ppermute(v, axis, RING4[1])


def down(v, axis):
    return lax.ppermute(v, axis, RING4[3])


def across(v, mask):
    if mask == 2:
        return lax.ppermute(v, "a", SWAP)
    if mask == 1:
        return lax.ppermute(v, "b", SWAP)
    return lax.ppermute(v, ("a", "b"), [(i, i ^ 3) for i in range(4)])


def ring_gather(block, axis):
    rows = block.shape[0] // 2
    lower = up(block, axis)
    upper = down(block, axis)
    top = up(lower[:rows], axis)
    bottom = down(upper[rows:], axis)
    return block, lower, upper, top, bottom


def params(limit=56 << 20):
    return pltpu.CompilerParams(vmem_limit_bytes=limit)


def assemble_tokens(place, own, rest):
    def body(place_ref, *refs):
        own_refs, rest_refs, (near, far) = refs[:5], refs[5:10], refs[10:]
        x = place_ref[0]
        for slot, shift in ((0, 0), (1, 3), (2, 1)):
            at = pl.multiple_of(((x + shift) % 4) * 384, 128)
            near[0:512, pl.ds(at, 384)] = own_refs[slot][...]
            near[512:1024, pl.ds(at, 384)] = rest_refs[slot][0:512, :]
            far[0:512, pl.ds(at, 384)] = rest_refs[slot][512:1024, :]
            far[512:1024, pl.ds(at, 384)] = rest_refs[slot][1024:1536, :]
        at = pl.multiple_of(((x + 2) % 4) * 384, 128)
        near[0:256, pl.ds(at, 384)] = own_refs[3][...]
        near[256:512, pl.ds(at, 384)] = own_refs[4][...]
        near[512:1024, pl.ds(at, 384)] = rest_refs[3][0:512, :]
        far[0:256, pl.ds(at, 384)] = rest_refs[3][512:768, :]
        far[256:512, pl.ds(at, 384)] = rest_refs[4][0:256, :]
        far[512:1024, pl.ds(at, 384)] = rest_refs[4][256:768, :]

    shape = jax.ShapeDtypeStruct((1024, 1536), jnp.bfloat16)
    return pl.pallas_call(
        body,
        out_shape=(shape, shape),
        in_specs=[SMEM] + [VMEM] * 10,
        out_specs=(VMEM, VMEM),
        compiler_params=params(),
        name="assemble_tokens",
    )(place, *own, *rest)


def near_sums(rows, blocks, width):
    def body(a, w0, w1, w2, top, bottom, out):
        def step(i, carry):
            at = pl.multiple_of(i * 256, 256)
            lhs = a[pl.ds(at, 256), :]
            for slot, ref in enumerate((w0, w1, w2)):
                out[slot, pl.ds(at, 256), :] = jnp.dot(lhs, ref[...], preferred_element_type=jnp.float32)
            out[3, pl.ds(at, 256), :] = jnp.dot(
                lhs[:, :768], top[...], preferred_element_type=jnp.float32
            ) + jnp.dot(lhs[:, 768:], bottom[...], preferred_element_type=jnp.float32)
            return carry

        lax.fori_loop(0, 4, step, 0)

    return pl.pallas_call(
        body,
        out_shape=jax.ShapeDtypeStruct((4, 1024, width), jnp.float32),
        in_specs=[VMEM] * 6,
        out_specs=VMEM,
        compiler_params=params(),
        name="near_sums",
    )(rows, *blocks)


def far_sums(place, sums, rows, blocks, width):
    def body(place_ref, s, a, w0, w1, w2, top, bottom, keep, send):
        z, b, c = place_ref[1], place_ref[2], place_ref[3]

        def step(i, carry):
            at = pl.multiple_of(i * 256, 256)
            lhs = a[pl.ds(at, 256), :]
            for slot, shift in ((0, 0), (1, 3), (2, 1), (3, 2)):
                if slot < 3:
                    total = jnp.dot(lhs, (w0, w1, w2)[slot][...], preferred_element_type=jnp.float32)
                else:
                    total = jnp.dot(
                        lhs[:, :768], top[...], preferred_element_type=jnp.float32
                    ) + jnp.dot(lhs[:, 768:], bottom[...], preferred_element_type=jnp.float32)
                total = total + s[slot, pl.ds(at, 256), :]
                owner = (z + shift) % 4
                place_at = (owner // 2 + b) % 2
                mine = owner % 2 == c

                @pl.when(mine)
                def _():
                    keep[place_at, pl.ds(at, 256), :] = total

                @pl.when(jnp.logical_not(mine))
                def _():
                    send[place_at, pl.ds(at, 256), :] = total

            return carry

        lax.fori_loop(0, 4, step, 0)

    shape = jax.ShapeDtypeStruct((2, 1024, width), jnp.float32)
    return pl.pallas_call(
        body,
        out_shape=(shape, shape),
        in_specs=[SMEM] + [VMEM] * 7,
        out_specs=(VMEM, VMEM),
        compiler_params=params(),
        name="far_sums",
    )(place, sums, rows, *blocks)


def lay_out(place, pieces):
    def body(place_ref, *refs):
        out = refs[-1]
        a, b = place_ref[4], place_ref[2]
        for h, (start, width) in enumerate(HALVES):
            for mask in range(4):
                fa, phi = (a + mask // 2) % 2, (b + mask % 2) % 2
                at = pl.multiple_of(fa * 768 + phi * 384 + start, 128)
                out[:, pl.ds(at, width)] = refs[h * 4 + mask][...]

    return pl.pallas_call(
        body,
        out_shape=jax.ShapeDtypeStruct((512, 1536), jnp.bfloat16),
        in_specs=[SMEM] + [VMEM] * 8,
        out_specs=VMEM,
        compiler_params=params(),
        name="lay_out",
    )(place, *pieces)


def per_device(tokens, weight, bias):
    x, z, a, b, c = (lax.axis_index(n) for n in ("x", "z", "a", "b", "c"))
    place = jnp.stack([x, z, b, c, a]).astype(jnp.int32)

    left, right = weight[:, :384], weight[:, 384:]
    first = b == 0
    own = [jnp.where(first, left[:, s : s + n], right[:, s : s + n]) for s, n in HALVES]
    give = [jnp.where(first, right[:, s : s + n], left[:, s : s + n]) for s, n in HALVES]

    near = [ring_gather(block, "z") for block in own]
    ta, tb, tab = (across(tokens, mask) for mask in (2, 1, 3))
    tok_own = ring_gather(tokens, "x")
    got = [across(block, 1) for block in give]
    tok_rest = ring_gather(jnp.concatenate([ta, tb, tab], 0), "x")
    far = [ring_gather(block, "z") for block in got]

    near_rows, far_rows = assemble_tokens(place, tok_own, tok_rest)

    mine = bias.reshape(2, 2, 384)
    theirs = lax.ppermute(bias, "b", SWAP).reshape(2, 2, 384)
    bias_at = jnp.stack([mine[a, b], theirs[a, b]])

    pieces = []
    for h, (start, width) in enumerate(HALVES):
        sums = near_sums(near_rows, near[h], width)
        keep, send = far_sums(place, sums, far_rows, far[h], width)
        other = lax.ppermute(send, "c", SWAP)
        pre = keep + other + bias_at[:, None, start : start + width]
        hidden = jax.nn.gelu(pre, approximate=False).astype(jnp.bfloat16)
        for mask in range(4):
            ra, rb = mask // 2, mask % 2
            block = hidden[rb, ra * 512 : (ra + 1) * 512, :]
            pieces.append(across(block, mask) if mask else block)
    return lay_out(place, pieces)


def solution(mesh):
    torus = Mesh(mesh.devices.reshape(4, 4, 2, 2, 2), ("x", "z", "a", "b", "c"))
    tokens_at = P(("z", "a"), ("b", "c", "x"))
    weight_at = P(("b", "c"), ("x", "z", "a"))
    bias_at = P(("x", "b", "c"))
    return jax.shard_map(
        per_device,
        mesh=torus,
        in_specs=(tokens_at, weight_at, bias_at),
        out_specs=P(("z", "a"), ("x", "b", "c")),
        check_vma=False,
    )
```

```python
import jax
import jax.numpy as jnp
from jax import lax
from jax.experimental import pallas as pl
from jax.experimental.pallas import tpu as pltpu
from jax.sharding import Mesh
from jax.sharding import PartitionSpec as P


NEAR = ((0, 256), (256, 128))
FAR = ((0, 0, 256), (1, 0, 128))
FORWARD = {"zn0": "both", "zn1": "both", "zf0": "both", "zf1": "both", "xo": "up", "xr1": "down", "xr2": "up"}
VMEM = pl.BlockSpec(memory_space=pltpu.VMEM)
ANY = pl.BlockSpec(memory_space=pl.ANY)
SWAP = [(0, 1), (1, 0)]


def shift(v, axis, step):
    return lax.ppermute(v, axis, [(i, (i + step) % 4) for i in range(4)])


def across(v, mask):
    if mask == 2:
        return lax.ppermute(v, "a", SWAP)
    if mask == 1:
        return lax.ppermute(v, "b", SWAP)
    return lax.ppermute(v, ("a", "b"), [(i, i ^ 3) for i in range(4)])


def places():
    return tuple(lax.axis_index(n) for n in ("x", "z", "a", "b", "c"))


def call(body, outs, vmem_args, extra=(), limit=4, scratch=(), out_spec=VMEM):
    args = [pltpu.with_memory_space_constraint(v, pltpu.VMEM) for v in vmem_args]
    return pl.pallas_call(
        body,
        out_shape=outs,
        in_specs=[VMEM] * len(args) + [ANY] * len(extra),
        out_specs=jax.tree.map(lambda _: out_spec, outs),
        scratch_shapes=scratch,
        compiler_params=pltpu.CompilerParams(vmem_limit_bytes=limit << 20),
    )(*args, *extra)


def vmem(shape, dtype):
    return pltpu.VMEM(shape, dtype)


def ring_gather(block, axis, tag):
    rows = block.shape[0] // 2
    lower = shift(block, axis, 1)
    upper = shift(block, axis, 3)
    mode = FORWARD[tag]
    if mode == "up":
        return block, lower, upper, shift(lower, axis, 1)
    if mode == "down":
        return block, lower, upper, shift(upper, axis, 3)

    def halves(low, upp, top, bottom):
        top[...] = low[0:rows, :]
        bottom[...] = upp[rows:, :]

    half = vmem((rows, block.shape[1]), block.dtype)
    top, bottom = call(halves, (half, half), [lower, upper])
    return block, lower, upper, shift(top, axis, 1), shift(bottom, axis, 3)


def prepare(weight, wanted):
    def body(w, *refs):
        outs, sems = refs[:-1], refs[-1]
        _, _, _, b, _ = places()
        copies = []
        for i, (own, start, width) in enumerate(wanted):
            at = pl.multiple_of((b if own else 1 - b) * 384 + start, 128)
            copies.append(pltpu.make_async_copy(w.at[:, pl.ds(at, width)], outs[i], sems.at[i]))
        for copy in copies:
            copy.start()
        for copy in copies:
            copy.wait()

    outs = tuple(vmem((1536, width), jnp.bfloat16) for _, _, width in wanted)
    weight = pltpu.with_memory_space_constraint(weight, pltpu.HBM)
    return call(body, outs, [], [weight], scratch=[pltpu.SemaphoreType.DMA((len(wanted),))])


def stack_rows(parts):
    def body(*refs):
        for i, ref in enumerate(refs[:-1]):
            refs[-1][i * 512 : (i + 1) * 512, :] = ref[...]

    return call(body, vmem((512 * len(parts), 384), jnp.bfloat16), parts)


def assemble(pieces, count):
    def body(*refs):
        ins, outs = refs[: len(pieces)], refs[len(pieces) :]
        x = places()[0]
        for step, group in ((0, ins[:1]), (3, ins[1:2]), (1, ins[2:3]), (2, ins[3:])):
            at = pl.multiple_of(((x + step) % 4) * 384, 128)
            row = 0
            for ref in group:
                for i, out in enumerate(outs):
                    first, last = max(row, i * 512), min(row + ref.shape[0], (i + 1) * 512)
                    if first < last:
                        out[first - i * 512 : last - i * 512, pl.ds(at, 384)] = ref[first - row : last - row, :]
                row += ref.shape[0]

    return call(body, (vmem((512, 1536), jnp.bfloat16),) * count, list(pieces))


def sides(w0, w1, w2, *w3):
    return (
        lambda: jnp.concatenate([w0[...], jnp.concatenate([w[...] for w in w3], 0) if len(w3) > 1 else w3[0][...]], 1),
        lambda: jnp.concatenate([w1[...], w2[...]], 1),
    )


def near_sums(rows, blocks, width):
    def body(a, *refs):
        blocks, out = refs[:-1], refs[-1]
        for i, side in enumerate(sides(*blocks)):
            out[i] = jnp.dot(a[...], side(), preferred_element_type=jnp.float32)

    return call(body, vmem((2, 512, 2 * width), jnp.float32), [rows, *blocks])


def far_sums(sums, rows, blocks, chunk):
    near, offset, width = chunk
    apart = NEAR[near][1]

    def body(s, a, *refs):
        blocks, keep, send = refs[:-2], refs[-2], refs[-1]
        _, z, _, b, c = places()
        even, odd = sides(*blocks)

        def fill(parity, side, owner, target):
            first = ((owner % 4) // 2 + b) % 2
            total = jnp.dot(a[...], side(), preferred_element_type=jnp.float32)
            target[first] = total[:, :width] + s[parity, :, offset : offset + width]
            target[1 - first] = total[:, width:] + s[parity, :, apart + offset : apart + offset + width]

        @pl.when(z % 2 == c)
        def _():
            fill(1, odd, z + 3, send)
            fill(0, even, z, keep)

        @pl.when(z % 2 != c)
        def _():
            fill(0, even, z, send)
            fill(1, odd, z + 3, keep)

    shape = vmem((2, 512, width), jnp.float32)
    return call(body, (shape, shape), [sums, rows, *blocks])


def activate(keep, other, mine, theirs, chunk):
    near, offset, width = chunk

    def body(k, o, bias_near, bias_far, *outs):
        _, _, a, b, _ = places()
        row = a * 6 + b * 3 + (NEAR[near][0] + offset) // 128
        for rb, bias_ref in enumerate((bias_near, bias_far)):
            for j in range(width // 128):
                cols = slice(j * 128, (j + 1) * 128)
                shift_by = bias_ref[pl.ds(row + j, 1), :]

                def step(i, carry):
                    at = pl.multiple_of(i * 64, 64)
                    v = k[rb, pl.ds(at, 64), cols] + o[rb, pl.ds(at, 64), cols] + shift_by
                    hidden = 0.5 * v * (1.0 + lax.erf(v * 0.7071067811865476))
                    outs[rb][pl.ds(at, 64), cols] = hidden.astype(jnp.bfloat16)
                    return carry

                lax.fori_loop(0, 8, step, 0)

    return call(body, (vmem((512, width), jnp.bfloat16),) * 2, [keep, other, mine, theirs])


def lay_out(pieces):
    def body(*refs):
        blocks, out, sems = refs[:-2], refs[-2], refs[-1]
        _, _, a, b, _ = places()
        copies = []
        for k, (near, offset, width) in enumerate(FAR):
            for mask in range(4):
                fa, phi = (a + mask // 2) % 2, (b + mask % 2) % 2
                at = pl.multiple_of(fa * 768 + phi * 384 + NEAR[near][0] + offset, 128)
                i = k * 4 + mask
                copies.append(pltpu.make_async_copy(blocks[i], out.at[:, pl.ds(at, width)], sems.at[i]))
        for copy in copies:
            copy.start()
        for copy in copies:
            copy.wait()

    out = jax.ShapeDtypeStruct((512, 1536), jnp.bfloat16)
    return call(body, out, pieces, scratch=[pltpu.SemaphoreType.DMA((len(pieces),))], out_spec=ANY)


def per_device_in_order(tokens, weight, bias):
    bias = bias.reshape(12, 128)
    own0 = prepare(weight, [(True, *NEAR[0])])
    spans = [(NEAR[near][0] + offset, width) for near, offset, width in FAR]
    own1, *give = prepare(weight, [(True, *NEAR[1])] + [(False, *span) for span in spans])

    near = [ring_gather(block, "z", f"zn{h}") for h, block in enumerate((*own0, own1))]
    ta, tb, tab = (across(tokens, mask) for mask in (2, 1, 3))
    tok_own = ring_gather(tokens, "x", "xo")
    got = [across(block, 1) for block in give]
    theirs = across(bias, 1)
    tok_one = ring_gather(stack_rows([ta, tab]), "x", "xr1")
    tok_two = ring_gather(tb, "x", "xr2")
    far = [ring_gather(block, "z", f"zf{k}") for k, block in enumerate(got)]

    (near_own,) = assemble(tok_own, 1)
    near_across, far_across = assemble(tok_one, 2)
    (far_own,) = assemble(tok_two, 1)
    sums = {}
    for h, (_, width) in enumerate(NEAR):
        for ra, rows in ((0, near_own), (1, near_across)):
            sums[h, ra] = near_sums(rows, near[h], width)

    pieces = []
    for k, chunk in enumerate(FAR):
        blocks = {}
        for ra, rows in ((1, far_across), (0, far_own)):
            keep, send = far_sums(sums[chunk[0], ra], rows, far[k], chunk)
            other = lax.ppermute(send, "c", SWAP)
            blocks[ra] = activate(keep, other, bias, theirs, chunk)
        pieces += [blocks[0][0], across(blocks[0][1], 1), across(blocks[1][0], 2), across(blocks[1][1], 3)]
    return lay_out(pieces)


def solution(mesh):
    torus = Mesh(mesh.devices.reshape(4, 4, 2, 2, 2), ("x", "z", "a", "b", "c"))
    tokens_at = P(("z", "a"), ("b", "c", "x"))
    weight_at = P(("b", "c"), ("x", "z", "a"))
    bias_at = P(("x", "b", "c"))
    return jax.shard_map(
        per_device_in_order,
        mesh=torus,
        in_specs=(tokens_at, weight_at, bias_at),
        out_specs=P(("z", "a"), ("x", "b", "c")),
        check_vma=False,
    )
```

```python
import jax
import jax.numpy as jnp
from jax import lax
from jax.experimental import pallas as pl
from jax.experimental.pallas import tpu as pltpu
from jax.sharding import Mesh
from jax.sharding import PartitionSpec as P


NEAR = ((0, 256), (256, 128))
FAR = ((0, 0, 256), (1, 0, 128))
FORWARD = {"zn0": "core", "zn1": "core", "zf0": "both", "zf1": "both", "xo": "core", "xr1": "core", "xr2": "core"}
VMEM = pl.BlockSpec(memory_space=pltpu.VMEM)
ANY = pl.BlockSpec(memory_space=pl.ANY)
SWAP = [(0, 1), (1, 0)]


def shift(v, axis, step):
    return lax.ppermute(v, axis, [(i, (i + step) % 4) for i in range(4)])


def across(v, mask):
    if mask == 2:
        return lax.ppermute(v, "a", SWAP)
    if mask == 1:
        return lax.ppermute(v, "b", SWAP)
    return lax.ppermute(v, ("a", "b"), [(i, i ^ 3) for i in range(4)])


def places():
    return tuple(lax.axis_index(n) for n in ("x", "z", "a", "b", "c"))


def call(body, outs, vmem_args, extra=(), limit=4, scratch=(), out_spec=VMEM, aliases=None):
    args = [pltpu.with_memory_space_constraint(v, pltpu.VMEM) for v in vmem_args]
    return pl.pallas_call(
        body,
        out_shape=outs,
        in_specs=[VMEM] * len(args) + [ANY] * len(extra),
        out_specs=jax.tree.map(lambda _: out_spec, outs),
        scratch_shapes=scratch,
        input_output_aliases=aliases or {},
        compiler_params=pltpu.CompilerParams(vmem_limit_bytes=limit << 20),
    )(*args, *extra)


def vmem(shape, dtype):
    return pltpu.VMEM(shape, dtype)


def ring_gather(block, axis, tag):
    rows = block.shape[0] // 2
    lower = shift(block, axis, 1)
    upper = shift(block, axis, 3)
    mode = FORWARD[tag]
    if mode == "core":

        def pick(low, upp, out):
            c = places()[4]

            @pl.when(c == 0)
            def _():
                out[...] = low[...]

            @pl.when(c != 0)
            def _():
                out[...] = upp[...]

        chosen = call(pick, vmem(block.shape, block.dtype), [lower, upper])
        pairs = [(2 * i + c, 2 * ((i + (1, 3)[c]) % 4) + c) for i in range(4) for c in (0, 1)]
        return block, lower, upper, lax.ppermute(chosen, (axis, "c"), pairs)
    if mode == "up":
        return block, lower, upper, shift(lower, axis, 1)
    if mode == "down":
        return block, lower, upper, shift(upper, axis, 3)

    def halves(low, upp, top, bottom):
        top[...] = low[0:rows, :]
        bottom[...] = upp[rows:, :]

    half = vmem((rows, block.shape[1]), block.dtype)
    top, bottom = call(halves, (half, half), [lower, upper])
    return block, lower, upper, shift(top, axis, 1), shift(bottom, axis, 3)


def prepare(weight, wanted):
    def body(w, *refs):
        outs, sems = refs[:-1], refs[-1]
        _, _, _, b, _ = places()
        copies = []
        for i, (own, start, width) in enumerate(wanted):
            at = pl.multiple_of((b if own else 1 - b) * 384 + start, 128)
            copies.append(pltpu.make_async_copy(w.at[:, pl.ds(at, width)], outs[i], sems.at[i]))
        for copy in copies:
            copy.start()
        for copy in copies:
            copy.wait()

    outs = tuple(vmem((1536, width), jnp.bfloat16) for _, _, width in wanted)
    weight = pltpu.with_memory_space_constraint(weight, pltpu.HBM)
    return call(body, outs, [], [weight], scratch=[pltpu.SemaphoreType.DMA((len(wanted),))])


def stack_rows(parts):
    def body(*refs):
        for i, ref in enumerate(refs[:-1]):
            refs[-1][i * 512 : (i + 1) * 512, :] = ref[...]

    return call(body, vmem((512 * len(parts), 384), jnp.bfloat16), parts)


def assemble(pieces, count):
    def body(*refs):
        ins, outs = refs[: len(pieces)], refs[len(pieces) :]
        x = places()[0]
        for step, group in ((0, ins[:1]), (3, ins[1:2]), (1, ins[2:3]), (2, ins[3:])):
            at = pl.multiple_of(((x + step) % 4) * 384, 128)
            row = 0
            for ref in group:
                for i, out in enumerate(outs):
                    first, last = max(row, i * 512), min(row + ref.shape[0], (i + 1) * 512)
                    if first < last:
                        out[first - i * 512 : last - i * 512, pl.ds(at, 384)] = ref[first - row : last - row, :]
                row += ref.shape[0]

    return call(body, (vmem((512, 1536), jnp.bfloat16),) * count, list(pieces))


def sides(w0, w1, w2, *w3):
    return (
        lambda: jnp.concatenate([w0[...], jnp.concatenate([w[...] for w in w3], 0) if len(w3) > 1 else w3[0][...]], 1),
        lambda: jnp.concatenate([w1[...], w2[...]], 1),
    )


def near_sums(rows, blocks, width):
    def body(a, *refs):
        blocks, out = refs[:-1], refs[-1]
        for i, side in enumerate(sides(*blocks)):
            out[i] = jnp.dot(a[...], side(), preferred_element_type=jnp.float32)

    return call(body, vmem((2, 512, 2 * width), jnp.float32), [rows, *blocks])


def far_sums(sums, rows, blocks, chunk):
    near, offset, width = chunk
    apart = NEAR[near][1]

    def body(s, a, *refs):
        blocks, keep, send = refs[:-2], refs[-2], refs[-1]
        _, z, _, b, c = places()
        even, odd = sides(*blocks)

        def fill(parity, side, owner, target):
            first = ((owner % 4) // 2 + b) % 2
            total = jnp.dot(a[...], side(), preferred_element_type=jnp.float32)
            target[first] = total[:, :width] + s[parity, :, offset : offset + width]
            target[1 - first] = total[:, width:] + s[parity, :, apart + offset : apart + offset + width]

        @pl.when(z % 2 == c)
        def _():
            fill(1, odd, z + 3, send)
            fill(0, even, z, keep)

        @pl.when(z % 2 != c)
        def _():
            fill(0, even, z, send)
            fill(1, odd, z + 3, keep)

    shape = vmem((2, 512, width), jnp.float32)
    return call(body, (shape, shape), [sums, rows, *blocks])


def activate(keep, other, mine, theirs, chunk):
    near, offset, width = chunk

    def body(k, o, bias_near, bias_far, *outs):
        _, _, a, b, _ = places()
        row = a * 6 + b * 3 + (NEAR[near][0] + offset) // 128
        for rb, bias_ref in enumerate((bias_near, bias_far)):
            for j in range(width // 128):
                cols = slice(j * 128, (j + 1) * 128)
                shift_by = bias_ref[pl.ds(row + j, 1), :]

                def step(i, carry):
                    at = pl.multiple_of(i * 64, 64)
                    v = k[rb, pl.ds(at, 64), cols] + o[rb, pl.ds(at, 64), cols] + shift_by
                    hidden = 0.5 * v * (1.0 + lax.erf(v * 0.7071067811865476))
                    outs[rb][pl.ds(at, 64), cols] = hidden.astype(jnp.bfloat16)
                    return carry

                lax.fori_loop(0, 8, step, 0)

    return call(body, (vmem((512, width), jnp.bfloat16),) * 2, [keep, other, mine, theirs])


def lay_out(pieces, chunk, filled=None):
    near, offset, width = chunk

    def body(*refs):
        blocks, out, sems = refs[:4], refs[-2], refs[-1]
        _, _, a, b, _ = places()
        copies = []
        for mask in range(4):
            fa, phi = (a + mask // 2) % 2, (b + mask % 2) % 2
            at = pl.multiple_of(fa * 768 + phi * 384 + NEAR[near][0] + offset, 128)
            copies.append(pltpu.make_async_copy(blocks[mask], out.at[:, pl.ds(at, width)], sems.at[mask]))
        for copy in copies:
            copy.start()
        for copy in copies:
            copy.wait()

    out = jax.ShapeDtypeStruct((512, 1536), jnp.bfloat16)
    scratch = [pltpu.SemaphoreType.DMA((4,))]
    extra, aliases = ([], {}) if filled is None else ([filled], {4: 0})
    return call(body, out, pieces, extra, scratch=scratch, out_spec=ANY, aliases=aliases)


def per_device_in_order(tokens, weight, bias):
    bias = bias.reshape(12, 128)
    own0 = prepare(weight, [(True, *NEAR[0])])
    spans = [(NEAR[near][0] + offset, width) for near, offset, width in FAR]
    own1, *give = prepare(weight, [(True, *NEAR[1])] + [(False, *span) for span in spans])

    near = [ring_gather(block, "z", f"zn{h}") for h, block in enumerate((*own0, own1))]
    ta, tb, tab = (across(tokens, mask) for mask in (2, 1, 3))
    tok_own = ring_gather(tokens, "x", "xo")
    got = [across(block, 1) for block in give]
    theirs = across(bias, 1)
    tok_one = ring_gather(stack_rows([ta, tab]), "x", "xr1")
    tok_two = ring_gather(tb, "x", "xr2")
    far = [ring_gather(block, "z", f"zf{k}") for k, block in enumerate(got)]

    (near_own,) = assemble(tok_own, 1)
    near_across, far_across = assemble(tok_one, 2)
    (far_own,) = assemble(tok_two, 1)
    sums = {}
    for h, (_, width) in enumerate(NEAR):
        for ra, rows in ((0, near_own), (1, near_across)):
            sums[h, ra] = near_sums(rows, near[h], width)

    hidden = None
    for k, chunk in enumerate(FAR):
        blocks = {}
        for ra, rows in ((1, far_across), (0, far_own)):
            keep, send = far_sums(sums[chunk[0], ra], rows, far[k], chunk)
            other = lax.ppermute(send, "c", SWAP)
            blocks[ra] = activate(keep, other, bias, theirs, chunk)
        pieces = [blocks[0][0], across(blocks[0][1], 1), across(blocks[1][0], 2), across(blocks[1][1], 3)]
        hidden = lay_out(pieces, chunk, hidden)
    return hidden


def solution(mesh):
    torus = Mesh(mesh.devices.reshape(4, 4, 2, 2, 2), ("x", "z", "a", "b", "c"))
    tokens_at = P(("z", "a"), ("b", "c", "x"))
    weight_at = P(("b", "c"), ("x", "z", "a"))
    bias_at = P(("x", "b", "c"))
    return jax.shard_map(
        per_device_in_order,
        mesh=torus,
        in_specs=(tokens_at, weight_at, bias_at),
        out_specs=P(("z", "a"), ("x", "b", "c")),
        check_vma=False,
    )
```

```python
import jax
import jax.numpy as jnp
from jax import lax
from jax.experimental import pallas as pl
from jax.experimental.pallas import tpu as pltpu
from jax.sharding import Mesh
from jax.sharding import PartitionSpec as P


NEAR = ((0, 256), (256, 128))
FAR = ((0, 0, 256), (1, 0, 128))
FORWARD = {"zn0": "core", "zn1": "core", "zf0": "both", "zf1": "both", "xo": "core", "xr1": "core", "xr2": "core"}
VMEM = pl.BlockSpec(memory_space=pltpu.VMEM)
ANY = pl.BlockSpec(memory_space=pl.ANY)
SWAP = [(0, 1), (1, 0)]


def shift(v, axis, step):
    return lax.ppermute(v, axis, [(i, (i + step) % 4) for i in range(4)])


def across(v, mask):
    if mask == 2:
        return lax.ppermute(v, "a", SWAP)
    if mask == 1:
        return lax.ppermute(v, "b", SWAP)
    return lax.ppermute(v, ("a", "b"), [(i, i ^ 3) for i in range(4)])


def places():
    return tuple(lax.axis_index(n) for n in ("x", "z", "a", "b", "c"))


def call(body, outs, vmem_args, extra=(), limit=4, scratch=(), out_spec=VMEM, aliases=None):
    args = [pltpu.with_memory_space_constraint(v, pltpu.VMEM) for v in vmem_args]
    return pl.pallas_call(
        body,
        out_shape=outs,
        in_specs=[VMEM] * len(args) + [ANY] * len(extra),
        out_specs=jax.tree.map(lambda _: out_spec, outs),
        scratch_shapes=scratch,
        input_output_aliases=aliases or {},
        compiler_params=pltpu.CompilerParams(vmem_limit_bytes=limit << 20),
    )(*args, *extra)


def vmem(shape, dtype):
    return pltpu.VMEM(shape, dtype)


def ring_gather(block, axis, tag):
    rows = block.shape[0] // 2
    lower = shift(block, axis, 1)
    upper = shift(block, axis, 3)
    mode = FORWARD[tag]
    if mode == "core":

        def pick(low, upp, out):
            c = places()[4]

            @pl.when(c == 0)
            def _():
                out[...] = low[...]

            @pl.when(c != 0)
            def _():
                out[...] = upp[...]

        chosen = call(pick, vmem(block.shape, block.dtype), [lower, upper])
        pairs = [(2 * i + c, 2 * ((i + (1, 3)[c]) % 4) + c) for i in range(4) for c in (0, 1)]
        return block, lower, upper, lax.ppermute(chosen, (axis, "c"), pairs)
    if mode == "up":
        return block, lower, upper, shift(lower, axis, 1)
    if mode == "down":
        return block, lower, upper, shift(upper, axis, 3)

    def halves(low, upp, top, bottom):
        top[...] = low[0:rows, :]
        bottom[...] = upp[rows:, :]

    half = vmem((rows, block.shape[1]), block.dtype)
    top, bottom = call(halves, (half, half), [lower, upper])
    return block, lower, upper, shift(top, axis, 1), shift(bottom, axis, 3)


def prepare(weight, wanted):
    def body(w, *refs):
        outs, sems = refs[:-1], refs[-1]
        _, _, _, b, _ = places()
        copies = []
        for i, (own, start, width) in enumerate(wanted):
            at = pl.multiple_of((b if own else 1 - b) * 384 + start, 128)
            copies.append(pltpu.make_async_copy(w.at[:, pl.ds(at, width)], outs[i], sems.at[i]))
        for copy in copies:
            copy.start()
        for copy in copies:
            copy.wait()

    outs = tuple(vmem((1536, width), jnp.bfloat16) for _, _, width in wanted)
    weight = pltpu.with_memory_space_constraint(weight, pltpu.HBM)
    return call(body, outs, [], [weight], scratch=[pltpu.SemaphoreType.DMA((len(wanted),))])


def stack_rows(parts):
    def body(*refs):
        for i, ref in enumerate(refs[:-1]):
            refs[-1][i * 512 : (i + 1) * 512, :] = ref[...]

    return call(body, vmem((512 * len(parts), 384), jnp.bfloat16), parts)


def assemble(pieces, count):
    def body(*refs):
        ins, outs = refs[: len(pieces)], refs[len(pieces) :]
        x = places()[0]
        for step, group in ((0, ins[:1]), (3, ins[1:2]), (1, ins[2:3]), (2, ins[3:])):
            at = pl.multiple_of(((x + step) % 4) * 384, 128)
            row = 0
            for ref in group:
                for i, out in enumerate(outs):
                    first, last = max(row, i * 512), min(row + ref.shape[0], (i + 1) * 512)
                    if first < last:
                        out[first - i * 512 : last - i * 512, pl.ds(at, 384)] = ref[first - row : last - row, :]
                row += ref.shape[0]

    return call(body, (vmem((512, 1536), jnp.bfloat16),) * count, list(pieces))


def sides(w0, w1, w2, *w3):
    return (
        lambda: jnp.concatenate([w0[...], jnp.concatenate([w[...] for w in w3], 0) if len(w3) > 1 else w3[0][...]], 1),
        lambda: jnp.concatenate([w1[...], w2[...]], 1),
    )


def near_sums(rows, blocks, width):
    def body(a, *refs):
        blocks, out = refs[:-1], refs[-1]
        for i, side in enumerate(sides(*blocks)):
            out[i] = jnp.dot(a[...], side(), preferred_element_type=jnp.float32)

    return call(body, vmem((2, 512, 2 * width), jnp.float32), [rows, *blocks])


def far_sums(sums, rows, blocks, chunk, keep):
    near, offset, width = chunk
    apart = NEAR[near][1]

    def body(s, a, *refs):
        blocks, out = refs[:-1], refs[-1]
        _, z, _, b, c = places()
        even, odd = sides(*blocks)

        def fill(parity, side, owner):
            first = ((owner % 4) // 2 + b) % 2
            total = jnp.dot(a[...], side(), preferred_element_type=jnp.float32)
            out[first] = total[:, :width] + s[parity, :, offset : offset + width]
            out[1 - first] = total[:, width:] + s[parity, :, apart + offset : apart + offset + width]

        @pl.when((z % 2 == c) == keep)
        def _():
            fill(0, even, z)

        @pl.when((z % 2 == c) != keep)
        def _():
            fill(1, odd, z + 3)

    return call(body, vmem((2, 512, width), jnp.float32), [sums, rows, *blocks])


def activate(keep, other, mine, theirs, chunk):
    near, offset, width = chunk

    def body(k, o, bias_near, bias_far, *outs):
        _, _, a, b, _ = places()
        row = a * 6 + b * 3 + (NEAR[near][0] + offset) // 128
        for rb, bias_ref in enumerate((bias_near, bias_far)):
            for j in range(width // 128):
                cols = slice(j * 128, (j + 1) * 128)
                shift_by = bias_ref[pl.ds(row + j, 1), :]

                def step(i, carry):
                    at = pl.multiple_of(i * 64, 64)
                    v = k[rb, pl.ds(at, 64), cols] + o[rb, pl.ds(at, 64), cols] + shift_by
                    hidden = 0.5 * v * (1.0 + lax.erf(v * 0.7071067811865476))
                    outs[rb][pl.ds(at, 64), cols] = hidden.astype(jnp.bfloat16)
                    return carry

                lax.fori_loop(0, 8, step, 0)

    return call(body, (vmem((512, width), jnp.bfloat16),) * 2, [keep, other, mine, theirs])


def lay_out(pieces, chunk, filled=None):
    near, offset, width = chunk

    def body(*refs):
        blocks, out, sems = refs[:4], refs[-2], refs[-1]
        _, _, a, b, _ = places()
        copies = []
        for mask in range(4):
            fa, phi = (a + mask // 2) % 2, (b + mask % 2) % 2
            at = pl.multiple_of(fa * 768 + phi * 384 + NEAR[near][0] + offset, 128)
            copies.append(pltpu.make_async_copy(blocks[mask], out.at[:, pl.ds(at, width)], sems.at[mask]))
        for copy in copies:
            copy.start()
        for copy in copies:
            copy.wait()

    out = jax.ShapeDtypeStruct((512, 1536), jnp.bfloat16)
    scratch = [pltpu.SemaphoreType.DMA((4,))]
    extra, aliases = ([], {}) if filled is None else ([filled], {4: 0})
    return call(body, out, pieces, extra, scratch=scratch, out_spec=ANY, aliases=aliases)


def per_device_in_order(tokens, weight, bias):
    bias = bias.reshape(12, 128)
    own0 = prepare(weight, [(True, *NEAR[0])])
    spans = [(NEAR[near][0] + offset, width) for near, offset, width in FAR]
    own1, *give = prepare(weight, [(True, *NEAR[1])] + [(False, *span) for span in spans])

    near = [ring_gather(block, "z", f"zn{h}") for h, block in enumerate((*own0, own1))]
    ta, tb, tab = (across(tokens, mask) for mask in (2, 1, 3))
    tok_own = ring_gather(tokens, "x", "xo")
    got = [across(block, 1) for block in give]
    theirs = across(bias, 1)
    tok_one = ring_gather(stack_rows([ta, tab]), "x", "xr1")
    tok_two = ring_gather(tb, "x", "xr2")
    far = [ring_gather(block, "z", f"zf{k}") for k, block in enumerate(got)]

    (near_own,) = assemble(tok_own, 1)
    near_across, far_across = assemble(tok_one, 2)
    (far_own,) = assemble(tok_two, 1)
    sums = {}
    for h, (_, width) in enumerate(NEAR):
        for ra, rows in ((0, near_own), (1, near_across)):
            sums[h, ra] = near_sums(rows, near[h], width)

    hidden = None
    for k, chunk in enumerate(FAR):
        blocks = {}
        for ra, rows in ((1, far_across), (0, far_own)):
            of = sums[chunk[0], ra], rows, far[k], chunk
            other = lax.ppermute(far_sums(*of, False), "c", SWAP)
            keep = far_sums(*of, True)
            blocks[ra] = activate(keep, other, bias, theirs, chunk)
        pieces = [blocks[0][0], across(blocks[0][1], 1), across(blocks[1][0], 2), across(blocks[1][1], 3)]
        hidden = lay_out(pieces, chunk, hidden)
    return hidden


def solution(mesh):
    torus = Mesh(mesh.devices.reshape(4, 4, 2, 2, 2), ("x", "z", "a", "b", "c"))
    tokens_at = P(("z", "a"), ("b", "c", "x"))
    weight_at = P(("b", "c"), ("x", "z", "a"))
    bias_at = P(("x", "b", "c"))
    return jax.shard_map(
        per_device_in_order,
        mesh=torus,
        in_specs=(tokens_at, weight_at, bias_at),
        out_specs=P(("z", "a"), ("x", "b", "c")),
        check_vma=False,
    )
```
